32 devices in a mesh: mesh: 8 (over z, x), col: 4 (over y, core).
Axes of the slice: x: 2, y: 2, z: 4, core: 2. Of those that a mesh axis runs over, the one named last changes fastest.
Arguments:
- x_cols: bfloat16 [32, 8192], P('col', 'mesh'), may hold values from -6 to 6
- q_tiles: bfloat16 [320, 128, 128], P('mesh'), may hold values from -0.25 to 0.25
- q_cols: int32 [64, 5], P('mesh'), may hold values from 0 to 15, as said below
- halo_ids: int32 [8, 2], P('mesh'), may hold values from 0 to 7
- a_tiles: bfloat16 [512, 128, 128], P('mesh'), may hold values from -0.1875 to 0.1875
- obs_prec: bfloat16 [512, 128], P('mesh'), may hold values from 0.5 to 4
- tile_owner: int32 [512, 1], P('mesh'), may hold values from 0 to 7; in each aligned block of 64 rows (0 to 63, 64 to 127, ...) at most 16 rows name the same one
- tile_sub: int32 [512], P('mesh'), may hold values from 0 to 7
Outputs:
- product: float32 [32, 8192], P('col', 'mesh')
- gram: float32 [32, 32], P(None, 'col')
The draws below stay inside these ranges and needn't reach their ends.
Inputs may be any that keep to these rules, and one draw needn't show every extreme that they name: `q_cols`: slot values index a partition's window of 16 row blocks as the first step defines. `tile_owner`: among the 64 tiles of one partition, no partition is named more than 16 times.
All inputs are finite; a program needn't handle non-finite values.
Results may differ from the reference program's by a relative error of at most 0.00081.
Values may be sent and summed in bfloat16 or wider, within the bound.
No kernel may reach another device: no remote copies, remote signals or barrier semaphores. Data moves between devices by JAX's collectives and lax.ppermute only.
A program may use at most 64 MiB of HBM per device.

```python
import math
import jax
import jax.numpy as jnp
import numpy as np
from jax import lax

TB = 128
COLS = 32
NB = 5
HALO = 2
RB_DEV = 8
OT_DEV = 64
PARTITIONS = 8
ROWBLOCKS = 64
NODES = 8192
OBS_TILES = 512
CAP = 16


def draw_q_cols(key, part):
    key_rotate, key_loose = jax.random.split(key, 2)
    row_ids = jnp.arange(ROWBLOCKS, dtype=jnp.int32)
    local_rows = row_ids % RB_DEV
    partition = row_ids // RB_DEV
    rotate = jax.random.randint(key_rotate, (PARTITIONS,), 0, 4 * HALO).astype(jnp.int32)[partition]
    entries = jnp.arange(1, NB, dtype=jnp.int32)
    order_idx = local_rows[:, None] * (NB - 1) + entries[None, :] - 1
    covered = RB_DEV + (order_idx + rotate[:, None]) % (4 * HALO)
    loose = jax.random.randint(key_loose, (ROWBLOCKS, NB - 1), 0, RB_DEV + 4 * HALO).astype(jnp.int32)
    extras = jnp.where(order_idx < 4 * HALO, covered, loose)
    return jnp.concatenate([local_rows[:, None], extras], axis=1).astype(jnp.int32)


def place_ends(result, rng, low, largest):
    spot = [jax.random.randint(jax.random.fold_in(rng, axis), (), 0, length) for axis, length in enumerate(result.shape)]
    main_axis = result.shape.index(max(result.shape))
    beside = spot[:main_axis] + [(spot[main_axis] + 1) % result.shape[main_axis]] + spot[main_axis + 1:]
    return result.at[tuple(spot)].set(low).at[tuple(beside)].set(largest)


def block_scale(rng, extent, cuts, smallest, largest):
    level, own = 1.0, jax.random.fold_in(rng, 6)
    for position, blocks in cuts:
        steps = jnp.exp(jax.random.uniform(jax.random.fold_in(own, position), (blocks,), jnp.float32, smallest / len(cuts), largest / len(cuts)))
        level = level * jnp.repeat(steps, extent[position] // blocks).reshape([-1 if axis == position else 1 for axis in range(len(extent))])
    return level


def shared_out(key, own, number, rows, amount, top, reach, lean):
    sequence = jax.random.permutation(key, amount)
    heavy_load, common = load_shares(amount, rows * top, reach, lean, True), load_shares(amount, rows * top, reach, lean, False)
    places = jnp.arange(amount)

    def named(sizes, offset_by):
        used = int((sizes > 0).sum())
        fixed = max(1, used // 4)
        passed = fixed + (places - fixed + offset_by * (used - fixed)) % max(1, amount - fixed)
        return jnp.zeros((amount,), jnp.int32).at[sequence[jnp.where(places < fixed, places, passed)]].set(jnp.asarray(sizes, jnp.int32))

    sizes = jnp.where(number % 4 == 0, named(heavy_load, number // 4), named(common, number - number // 4 - 1))
    mixed = jax.random.permutation(jax.random.fold_in(own, 3), amount)
    giver, receiver = mixed[0:amount // 2 * 2:2], mixed[1:amount // 2 * 2:2]
    slack = jnp.minimum(sizes[giver] - 1, reach - sizes[receiver]) // 2
    slack = jnp.where((giver == sequence[0]) | (receiver == sequence[0]) | (sizes[receiver] == 0), 0, jnp.maximum(slack, 0))
    passed = jax.random.randint(jax.random.fold_in(own, 4), (amount // 2,), 0, 1 << 20) % (slack + 1)
    sizes = sizes.at[giver].add(-passed).at[receiver].add(passed)
    members = jnp.searchsorted(jnp.cumsum(sizes), jnp.arange(rows * top), side="right").astype(jnp.int32)
    table = members.reshape(top, rows).T
    table = table[jax.random.permutation(jax.random.fold_in(own, 1), rows)]
    offset_by = jax.random.randint(jax.random.fold_in(own, 2), (rows, 1), 0, top)
    return jnp.take_along_axis(table, (jnp.arange(top)[None, :] + offset_by) % top, axis=1)


def load_shares(count, total, reach, lean, full):
    loads = [(1 << 20) // math.isqrt(standing ** lean) + 1 for standing in range(1, count + 1)]
    largest = reach if full else min(reach, max(-(-total // count), total * loads[0] // sum(loads)))
    least = 1 if total - largest >= count - 1 else 0
    counts, surplus = [largest] + [least] * (count - 1), total - largest - least * (count - 1)
    while surplus > 0:
        movable = [i for i in range(1, count) if counts[i] < largest] or [i for i in range(1, count) if counts[i] < reach]
        pool, budget = sum([loads[i] for i in movable]), surplus
        for i in movable:
            addition = min(reach - counts[i], max(1, budget * loads[i] // pool), surplus)
            counts[i] = counts[i] + addition
            surplus = surplus - addition
    return np.array(counts)


def bell_draw(key, shape, deviation, limit, cuts=(), kind=jnp.bfloat16):
    values = deviation * jax.random.normal(key, shape, jnp.float32)
    if cuts:
        values = values * block_scale(key, shape, cuts, -0.22, 0.18)
    return jnp.clip(values, -limit, limit).astype(kind)


def setup_inputs(seed: int = 0) -> dict:
    arg_keys = jax.random.split(jax.random.key(seed), 9)
    x_cols = bell_draw(arg_keys[0], (COLS, NODES), 1.0, 6.0, ((0, 4), (1, 8)))
    q_tiles = bell_draw(arg_keys[1], (ROWBLOCKS * NB, TB, TB), (NB * TB) ** -0.5, 0.25, ((0, 8),))
    q_cols = draw_q_cols(jax.random.fold_in(arg_keys[8], 71), 0)
    halo_ids = place_ends(jax.random.randint(arg_keys[3], (PARTITIONS, HALO), 0, RB_DEV), jax.random.fold_in(arg_keys[3], 1), 0, RB_DEV - 1).astype(jnp.int32)
    a_tiles = bell_draw(arg_keys[4], (OBS_TILES, TB, TB), (8 * TB) ** -0.5, 0.1875, ((0, 8),))
    obs_prec = jnp.clip(jnp.exp(math.log(4.0) - 2.0794415 * jax.random.uniform(arg_keys[5], (OBS_TILES, TB), jnp.float32) ** block_scale(arg_keys[5], (OBS_TILES, TB), ((0, 8),), -0.2, 0.2)), 0.5, 4.0).astype(jnp.bfloat16)
    tile_owner_keys = jax.random.split(jax.random.fold_in(arg_keys[6], 1), OBS_TILES // OT_DEV)
    tile_owner_turns = jax.random.permutation(jax.random.fold_in(arg_keys[6], 3), OBS_TILES // OT_DEV)
    tile_owner = jax.vmap(lambda own, number: shared_out(jax.random.fold_in(arg_keys[6], 2), own, number, OT_DEV, PARTITIONS, 1, CAP, 2))(tile_owner_keys, tile_owner_turns).reshape((OBS_TILES, 1))
    tile_sub = place_ends(jax.random.randint(arg_keys[7], (OBS_TILES,), 0, RB_DEV), jax.random.fold_in(arg_keys[7], 1), 0, RB_DEV - 1).astype(jnp.int32)
    return {"x_cols": x_cols, "q_tiles": q_tiles, "q_cols": q_cols, "halo_ids": halo_ids, "a_tiles": a_tiles, "obs_prec": obs_prec, "tile_owner": tile_owner, "tile_sub": tile_sub}


HIGHEST = lax.Precision.HIGHEST
OFFSETS = (-2, -1, 1, 2)

def window_blocks(q_cols, halo_ids):
    row_ids = jnp.arange(ROWBLOCKS, dtype=jnp.int32)
    partition = (row_ids // RB_DEV)[:, None]
    beyond = jnp.maximum(q_cols - RB_DEV, 0)
    halo_side = beyond // HALO
    halo_slot = beyond % HALO
    offset = jnp.array(OFFSETS, dtype=jnp.int32)[halo_side]
    source_part = (partition + offset) % PARTITIONS
    remote = source_part * RB_DEV + halo_ids[source_part, halo_slot]
    return jnp.where(q_cols < RB_DEV, partition * RB_DEV + q_cols, remote).astype(jnp.int32)

def tile_terms(obs_tiles, precisions, x_blocks):
    wide_tiles = obs_tiles.astype(jnp.float32)
    projected = jnp.einsum('ton,tcn->tco', wide_tiles, x_blocks.astype(jnp.float32), precision=HIGHEST)
    weighted = (precisions.astype(jnp.float32)[:, None, :] * projected).astype(jnp.bfloat16)
    return jnp.einsum('ton,tco->tcn', wide_tiles, weighted.astype(jnp.float32), precision=HIGHEST)

def reference(x_cols, q_tiles, q_cols, halo_ids, a_tiles, obs_prec, tile_owner, tile_sub):
    blocks = x_cols.reshape(COLS, ROWBLOCKS, TB).transpose(1, 0, 2)
    sources = window_blocks(q_cols, halo_ids).reshape(PARTITIONS, RB_DEV * NB)
    q_grouped = q_tiles.reshape(PARTITIONS, RB_DEV * NB, TB, TB)

    def prior_part(paired):
        q_block, block_ids = paired
        x_blocks = blocks[block_ids].astype(jnp.float32)
        partial_value = jnp.einsum('kij,kcj->kci', q_block.astype(jnp.float32), x_blocks, precision=HIGHEST)
        return partial_value.reshape(RB_DEV, NB, COLS, TB).sum(axis=1)
    prior = lax.map(prior_part, (q_grouped, sources)).reshape(ROWBLOCKS, COLS, TB)
    targets = (tile_owner[:, 0] * RB_DEV + tile_sub).astype(jnp.int32).reshape(PARTITIONS, OT_DEV)

    def add_obs(running, paired):
        obs_tiles, precisions, block_ids = paired
        contrib = tile_terms(obs_tiles, precisions, blocks[block_ids])
        return (running.at[block_ids].add(contrib), None)
    start = jnp.zeros((ROWBLOCKS, COLS, TB), jnp.float32)
    observed, _ = lax.scan(add_obs, start, (a_tiles.reshape(PARTITIONS, OT_DEV, TB, TB), obs_prec.reshape(PARTITIONS, OT_DEV, TB), targets))
    combined = prior + observed
    product = combined.transpose(1, 0, 2).reshape(COLS, NODES)
    gram = jnp.dot(x_cols.astype(jnp.float32), product.T, precision=HIGHEST) / math.sqrt(NODES)
    return (product, gram)
```

```python
import math

import jax
import jax.numpy as jnp
from jax import lax
from jax.experimental import pallas as pl
from jax.experimental.pallas import tpu as pltpu
from jax.sharding import PartitionSpec as P

OFFSETS = (-2, -1, 1, 2)
LANES = 128
NT = (((1,), (1,)), ((), ()))
UNROLL = 16
GRANT = 16 * 2**20


def offer_kernel(halo_ids, x_cols, offered):
    parts, cols, width = offered.shape
    nodes = width - LANES
    rows = lax.broadcasted_iota(jnp.int32, (cols, LANES), 0)
    ids = jnp.zeros((cols, LANES), jnp.float32)
    for j in range(halo_ids.shape[1]):
        ids = jnp.where(rows == j, halo_ids[0, j].astype(jnp.float32), ids)
    ids = ids.astype(offered.dtype)
    own = x_cols[...]

    def put(part, carry):
        offered[part, :, :nodes] = own
        offered[part, :, nodes:] = ids
        return carry

    lax.fori_loop(0, parts, put, 0)


def terms_kernel(
    owners, subs, q_cols, xg, a_tiles, precisions, q_tiles, message, window, weighted
):
    parts, cols, width = xg.shape
    obs_count, tile, _ = a_tiles.shape
    row_blocks, neighbours = q_cols.shape
    nodes = row_blocks * tile
    halo = (window.shape[0] - row_blocks) // len(OFFSETS)
    me = lax.axis_index("mesh")

    def block(part, row):
        return xg[part, :, pl.ds(pl.multiple_of(row * tile, tile), tile)]

    for row in range(row_blocks):
        window[row] = xg[me, :, row * tile:(row + 1) * tile]
    for m, offset in enumerate(OFFSETS):
        part = lax.rem(me + offset + parts, parts)
        ids = xg[part, :, nodes:nodes + tile].astype(jnp.float32)
        for j in range(halo):
            wanted = jnp.broadcast_to(ids[j:j + 1, :], (cols, tile))
            picked = jnp.zeros((cols, tile), jnp.float32)
            for row in range(row_blocks):
                picked = jnp.where(
                    wanted == float(row),
                    xg[part, :, row * tile:(row + 1) * tile].astype(jnp.float32),
                    picked,
                )
            window[row_blocks + m * halo + j] = picked.astype(jnp.bfloat16)

    message[...] = jnp.zeros_like(message)

    def project(step, carry):
        first = pl.multiple_of(step * UNROLL, UNROLL)
        scales = precisions[pl.ds(first, UNROLL), :].astype(jnp.float32)
        for u in range(UNROLL):
            t = step * UNROLL + u
            projected = lax.dot_general(
                block(owners[t], subs[t]), a_tiles[t], NT, preferred_element_type=jnp.float32
            )
            weighted[t] = (scales[u:u + 1, :] * projected).astype(jnp.bfloat16)
        return carry

    lax.fori_loop(0, obs_count // UNROLL, project, 0)

    for row in range(row_blocks):
        total = None
        for k in range(neighbours):
            term = lax.dot_general(
                window[q_cols[row, k]], q_tiles[row * neighbours + k], NT,
                preferred_element_type=jnp.float32,
            )
            total = term if total is None else total + term
        message[me, :, row * tile:(row + 1) * tile] = total

    def spread(step, carry):
        made = [
            jnp.dot(weighted[step * UNROLL + u], a_tiles[step * UNROLL + u],
                    preferred_element_type=jnp.float32)
            for u in range(UNROLL)
        ]
        for u in range(UNROLL):
            t = step * UNROLL + u
            lanes = pl.ds(pl.multiple_of(subs[t] * tile, tile), tile)
            message[owners[t], :, lanes] = message[owners[t], :, lanes] + made[u]
        return carry

    lax.fori_loop(0, obs_count // UNROLL, spread, 0)


def gram_kernel(sent, own, near1, near2, near3, message):
    parts, cols, width = own.shape
    nodes = width - LANES
    mine = lax.axis_index("col")
    total = jnp.zeros((cols, LANES), jnp.float32)
    pieces = [None] * 4

    def add(part, carry):
        value = sent[part, :, :nodes]
        high = value.astype(jnp.bfloat16)
        low = (value - high.astype(jnp.float32)).astype(jnp.bfloat16)
        out = []
        for ref, old in zip((own, near1, near2, near3), carry):
            x = ref[part, :, :nodes]
            out.append(
                old
                + lax.dot_general(high, x, NT, preferred_element_type=jnp.float32)
                + lax.dot_general(low, x, NT, preferred_element_type=jnp.float32)
            )
        return tuple(out)

    pieces = tuple(jnp.zeros((cols, cols), jnp.float32) for _ in range(4))
    if parts <= 16:
        for part in range(parts):
            pieces = add(part, pieces)
    else:
        pieces = lax.fori_loop(0, parts, add, pieces)
    for k, piece in enumerate(pieces):
        wide = jnp.concatenate([piece, jnp.zeros((cols, LANES - cols), jnp.float32)], axis=1)
        total = total + pltpu.roll(wide, lax.bitwise_xor(mine, k) * cols, 1)

    def put(part, carry):
        message[part, :, nodes:] = total
        return carry

    lax.fori_loop(0, parts, put, 0)


def body(x_cols, q_tiles, q_cols, halo_ids, a_tiles, obs_prec, tile_owner, tile_sub):
    cols, nodes = x_cols.shape
    parts, groups = lax.axis_size("mesh"), lax.axis_size("col")
    obs_count, tile, _ = a_tiles.shape
    row_blocks = nodes // tile
    halo = halo_ids.shape[1]
    width = nodes + LANES
    vmem, smem = pl.BlockSpec(memory_space=pltpu.VMEM), pl.BlockSpec(memory_space=pltpu.SMEM)
    offered = pl.pallas_call(
        offer_kernel,
        out_shape=jax.ShapeDtypeStruct((parts, cols, width), x_cols.dtype),
        in_specs=[smem, vmem],
        out_specs=vmem,
        compiler_params=pltpu.CompilerParams(vmem_limit_bytes=GRANT),
        name="offer",
    )(halo_ids, x_cols)
    xg = lax.all_to_all(offered, "mesh", 0, 0, tiled=True)
    near = [
        lax.ppermute(xg, "col", [(i, i ^ k) for i in range(groups)]) for k in range(1, groups)
    ]
    shape = jax.ShapeDtypeStruct((parts, cols, width), jnp.float32)
    message = pl.pallas_call(
        terms_kernel,
        out_shape=shape,
        in_specs=[smem, smem, smem, vmem, vmem, vmem, vmem],
        out_specs=vmem,
        scratch_shapes=[
            pltpu.VMEM((row_blocks + len(OFFSETS) * halo, cols, tile), jnp.bfloat16),
            pltpu.VMEM((obs_count, cols, tile), jnp.bfloat16),
        ],
        cost_estimate=pl.CostEstimate(
            flops=60_000_000, bytes_accessed=4_000_000, transcendentals=0
        ),
        compiler_params=pltpu.CompilerParams(vmem_limit_bytes=GRANT),
        name="terms",
    )(tile_owner.reshape(-1), tile_sub, q_cols, xg, a_tiles, obs_prec, q_tiles)
    message = pl.pallas_call(
        gram_kernel,
        out_shape=shape,
        in_specs=[vmem] * 5,
        out_specs=vmem,
        input_output_aliases={0: 0},
        cost_estimate=pl.CostEstimate(
            flops=10_000_000, bytes_accessed=1_000_000, transcendentals=0
        ),
        compiler_params=pltpu.CompilerParams(vmem_limit_bytes=GRANT),
        name="gram",
    )(message, xg, *near)
    arrived = lax.all_to_all(message, "mesh", 0, 0, tiled=True)
    summed = jnp.sum(arrived, axis=0)
    gram = summed[:, nodes:nodes + groups * cols].T / math.sqrt(nodes * parts)
    return summed[:, :nodes], gram


def solution(mesh):
    placed = (
        P("col", "mesh"),
        P("mesh", None, None),
        P("mesh", None),
        P("mesh", None),
        P("mesh", None, None),
        P("mesh", None),
        P("mesh", None),
        P("mesh"),
    )
    return jax.shard_map(
        body,
        mesh=mesh,
        in_specs=placed,
        out_specs=(P("col", "mesh"), P(None, "col")),
        check_vma=False,
    )
```

```python
import math

import jax
import jax.numpy as jnp
from jax import lax
from jax.experimental import pallas as pl
from jax.experimental.pallas import tpu as pltpu
from jax.sharding import PartitionSpec as P

OFFSETS = (-2, -1, 1, 2)
LANES = 128
NT = (((1,), (1,)), ((), ()))
UNROLL = 16
GRANT = 16 * 2**20


def offer_kernel(halo_ids, x_cols, offered, ids_here, ids_sem, x_sems):
    parts, cols, width = offered.shape
    nodes = width - LANES
    copies = [
        pltpu.make_async_copy(x_cols, offered.at[part, :, pl.ds(0, nodes)], x_sems.at[part])
        for part in range(parts)
    ]
    fetch = pltpu.make_async_copy(halo_ids, ids_here, ids_sem)
    fetch.start()
    for copy in copies:
        copy.start()
    fetch.wait()
    rows = lax.broadcasted_iota(jnp.int32, (cols, LANES), 0)
    ids = jnp.zeros((cols, LANES), jnp.float32)
    for j in range(halo_ids.shape[1]):
        ids = jnp.where(rows == j, ids_here[0, j].astype(jnp.float32), ids)
    ids = ids.astype(offered.dtype)
    for part in range(parts):
        offered[part, :, nodes:] = ids
    for copy in copies:
        copy.wait()


def project_kernel(
    owners, subs, q_cols, xg, a_tiles, precisions, q_tiles, weighted, prior, window
):
    parts, cols, width = xg.shape
    obs_count, tile, _ = a_tiles.shape
    row_blocks, neighbours = q_cols.shape
    nodes = row_blocks * tile
    halo = (window.shape[0] - row_blocks) // len(OFFSETS)
    me = lax.axis_index("mesh")

    for row in range(row_blocks):
        window[row] = xg[me, :, row * tile:(row + 1) * tile]
    for m, offset in enumerate(OFFSETS):
        part = lax.rem(me + offset + parts, parts)
        ids = xg[part, :, nodes:nodes + tile].astype(jnp.float32)
        for j in range(halo):
            wanted = jnp.broadcast_to(ids[j:j + 1, :], (cols, tile))
            picked = jnp.zeros((cols, tile), jnp.float32)
            for row in range(row_blocks):
                picked = jnp.where(
                    wanted == float(row),
                    xg[part, :, row * tile:(row + 1) * tile].astype(jnp.float32),
                    picked,
                )
            window[row_blocks + m * halo + j] = picked.astype(jnp.bfloat16)

    def project(step, carry):
        first = pl.multiple_of(step * UNROLL, UNROLL)
        scales = precisions[pl.ds(first, UNROLL), :].astype(jnp.float32)
        for u in range(UNROLL):
            t = step * UNROLL + u
            lanes = pl.ds(pl.multiple_of(subs[t] * tile, tile), tile)
            projected = lax.dot_general(
                xg[owners[t], :, lanes], a_tiles[t], NT, preferred_element_type=jnp.float32
            )
            weighted[t] = (scales[u:u + 1, :] * projected).astype(jnp.bfloat16)
        return carry

    lax.fori_loop(0, obs_count // UNROLL, project, 0)

    for row in range(row_blocks):
        total = None
        for k in range(neighbours):
            term = lax.dot_general(
                window[q_cols[row, k]], q_tiles[row * neighbours + k], NT,
                preferred_element_type=jnp.float32,
            )
            total = term if total is None else total + term
        prior[:, row * tile:(row + 1) * tile] = total


def spread_kernel(owners, subs, weighted, a_tiles, prior, summed):
    obs_count, tile, _ = a_tiles.shape
    summed[...] = jnp.zeros_like(summed)
    summed[lax.axis_index("mesh")] = prior[...]

    def spread(step, carry):
        made = [
            jnp.dot(weighted[step * UNROLL + u], a_tiles[step * UNROLL + u],
                    preferred_element_type=jnp.float32)
            for u in range(UNROLL)
        ]
        for u in range(UNROLL):
            t = step * UNROLL + u
            lanes = pl.ds(pl.multiple_of(subs[t] * tile, tile), tile)
            summed[owners[t], :, lanes] = summed[owners[t], :, lanes] + made[u]
        return carry

    lax.fori_loop(0, obs_count // UNROLL, spread, 0)


def over_parts(parts, step, carry):
    if parts > 16:
        return lax.fori_loop(0, parts, step, carry)
    for part in range(parts):
        carry = step(part, carry)
    return carry


def top_exponent(value):
    top = jnp.maximum(jnp.max(jnp.abs(value), axis=1, keepdims=True), 1e-30)
    return jnp.floor(jnp.log(32000.0 / top) * (1.0 / math.log(2.0)))


def power(exponent):
    return jnp.exp2(exponent)


def whole(value):
    return jnp.round(value).astype(jnp.int32).astype(jnp.int16)


def gram_kernel(summed, own, near1, near2, near3, message):
    parts, cols, nodes = summed.shape
    mine = lax.axis_index("col")

    def add(part, carry):
        value = summed[part]
        high = value.astype(jnp.bfloat16)
        low = (value - high.astype(jnp.float32)).astype(jnp.bfloat16)
        out = []
        for ref, old in zip((own, near1, near2, near3), carry):
            x = ref[part, :, :nodes]
            out.append(
                old
                + lax.dot_general(high, x, NT, preferred_element_type=jnp.float32)
                + lax.dot_general(low, x, NT, preferred_element_type=jnp.float32)
            )
        return tuple(out)

    pieces = over_parts(parts, add, (jnp.zeros((cols, cols), jnp.float32),) * 4)
    total = jnp.zeros((cols, LANES), jnp.float32)
    for k, piece in enumerate(pieces):
        wide = jnp.concatenate([piece, jnp.zeros((cols, LANES - cols), jnp.float32)], axis=1)
        total = total + pltpu.roll(wide, lax.bitwise_xor(mine, k) * cols, 1)

    quarter = LANES // 4
    lane = lax.broadcasted_iota(jnp.int32, (cols, LANES), 1)
    gram_exponent = top_exponent(total)
    scaled = total * power(gram_exponent)
    first = jnp.round(scaled)
    second = pltpu.roll((scaled - first) * 32768.0, quarter, 1)
    extra = jnp.where(lane < quarter, first, jnp.where(lane < 2 * quarter, second, gram_exponent))

    def put(part, carry):
        value = summed[part]
        exponent = top_exponent(value)
        message[part, :, :nodes] = whole(value * power(exponent))
        message[part, :, nodes:] = whole(jnp.where(lane < 3 * quarter, extra, exponent))
        return carry

    over_parts(parts, put, 0)


def collect_kernel(summed, arrived, product, gram):
    parts, cols, nodes = summed.shape
    quarter = LANES // 4
    me = lax.axis_index("mesh")

    def add(part, carry):
        total, pairs = carry
        extra = arrived[part, :, nodes:].astype(jnp.int32).astype(jnp.float32)
        back = power(-extra[:, 3 * quarter:3 * quarter + 1])
        here = arrived[part, :, :nodes].astype(jnp.int32).astype(jnp.float32) * back
        total = total + jnp.where(part == me, summed[part], here)
        values = extra + pltpu.roll(extra, LANES - quarter, 1) * (1.0 / 32768.0)
        return total, pairs + values * power(-extra[:, 2 * quarter:2 * quarter + 1])

    start = jnp.zeros((cols, nodes), jnp.float32), jnp.zeros((cols, LANES), jnp.float32)
    total, pairs = over_parts(parts, add, start)
    product[...] = total
    gram[...] = pairs[:, :gram.shape[1]] * (1.0 / math.sqrt(nodes * parts))


def body(x_cols, q_tiles, q_cols, halo_ids, a_tiles, obs_prec, tile_owner, tile_sub):
    cols, nodes = x_cols.shape
    parts, groups = lax.axis_size("mesh"), lax.axis_size("col")
    obs_count, tile, _ = a_tiles.shape
    row_blocks = nodes // tile
    halo = halo_ids.shape[1]
    width = nodes + LANES
    vmem, smem = pl.BlockSpec(memory_space=pltpu.VMEM), pl.BlockSpec(memory_space=pltpu.SMEM)
    hbm = pl.BlockSpec(memory_space=pltpu.HBM)
    offered = pl.pallas_call(
        offer_kernel,
        out_shape=jax.ShapeDtypeStruct((parts, cols, width), x_cols.dtype),
        in_specs=[hbm, hbm],
        out_specs=vmem,
        scratch_shapes=[
            pltpu.SMEM(halo_ids.shape, jnp.int32),
            pltpu.SemaphoreType.DMA,
            pltpu.SemaphoreType.DMA((parts,)),
        ],
        compiler_params=pltpu.CompilerParams(vmem_limit_bytes=GRANT),
        cost_estimate=pl.CostEstimate(
            flops=2_000_000_000, bytes_accessed=200_000, transcendentals=0
        ),
        name="offer",
    )(*(pltpu.with_memory_space_constraint(a, pltpu.HBM) for a in (halo_ids, x_cols)))
    xg = lax.all_to_all(offered, "mesh", 0, 0, tiled=True)
    def swap(array, k):
        return lax.ppermute(array, "col", [(i, i ^ k) for i in range(groups)])

    near2 = swap(xg, 2)
    near1 = swap(xg, 1)
    params = pltpu.CompilerParams(vmem_limit_bytes=GRANT)
    owners = tile_owner.reshape(-1)
    weighted, prior = pl.pallas_call(
        project_kernel,
        out_shape=[
            jax.ShapeDtypeStruct((obs_count, cols, tile), jnp.bfloat16),
            jax.ShapeDtypeStruct((cols, nodes), jnp.float32),
        ],
        in_specs=[smem, smem, smem, vmem, vmem, vmem, vmem],
        out_specs=[vmem, vmem],
        scratch_shapes=[pltpu.VMEM((row_blocks + len(OFFSETS) * halo, cols, tile), jnp.bfloat16)],
        compiler_params=params,
        cost_estimate=pl.CostEstimate(
            flops=60_000_000, bytes_accessed=4_000_000, transcendentals=0
        ),
        name="project",
    )(owners, tile_sub, q_cols, xg, a_tiles, obs_prec, q_tiles)
    near2, weighted = lax.optimization_barrier((near2, weighted))
    near3 = swap(near2, 1)
    summed = pl.pallas_call(
        spread_kernel,
        out_shape=jax.ShapeDtypeStruct((parts, cols, nodes), jnp.float32),
        in_specs=[smem, smem, vmem, vmem, vmem],
        out_specs=vmem,
        compiler_params=params,
        cost_estimate=pl.CostEstimate(
            flops=60_000_000, bytes_accessed=4_000_000, transcendentals=0
        ),
        name="spread",
    )(owners, tile_sub, weighted, a_tiles, prior)
    message = pl.pallas_call(
        gram_kernel,
        out_shape=jax.ShapeDtypeStruct((parts, cols, width), jnp.int16),
        in_specs=[vmem] * 5,
        out_specs=vmem,
        compiler_params=params,
        cost_estimate=pl.CostEstimate(
            flops=10_000_000, bytes_accessed=1_000_000, transcendentals=0
        ),
        name="gram",
    )(summed, xg, near1, near2, near3)
    arrived = lax.all_to_all(message, "mesh", 0, 0, tiled=True)
    product, gram = pl.pallas_call(
        collect_kernel,
        out_shape=[
            jax.ShapeDtypeStruct((cols, nodes), jnp.float32),
            jax.ShapeDtypeStruct((cols, groups * cols), jnp.float32),
        ],
        in_specs=[vmem, vmem],
        out_specs=[vmem, vmem],
        compiler_params=params,
        name="collect",
    )(summed, arrived)
    return product, gram.T


def solution(mesh):
    placed = (
        P("col", "mesh"),
        P("mesh", None, None),
        P("mesh", None),
        P("mesh", None),
        P("mesh", None, None),
        P("mesh", None),
        P("mesh", None),
        P("mesh"),
    )
    return jax.shard_map(
        body,
        mesh=mesh,
        in_specs=placed,
        out_specs=(P("col", "mesh"), P(None, "col")),
        check_vma=False,
    )
```

```python
import math

import jax
import jax.numpy as jnp
from jax import lax
from jax.experimental import pallas as pl
from jax.experimental.pallas import tpu as pltpu
from jax.sharding import PartitionSpec as P

OFFSETS = (-2, -1, 1, 2)
LANES = 128
NT = (((1,), (1,)), ((), ()))
UNROLL = 64
GRANT = 16 * 2**20


def offer_kernel(halo_ids, x_cols, offered, ids_here, x_here, sems):
    parts, cols, width = offered.shape
    nodes = width - LANES
    fetch_ids = pltpu.make_async_copy(halo_ids, ids_here, sems.at[0])
    fetch_x = pltpu.make_async_copy(x_cols, x_here, sems.at[1])
    fetch_ids.start()
    fetch_x.start()
    fetch_ids.wait()
    rows = lax.broadcasted_iota(jnp.int32, (cols, LANES), 0)
    ids = jnp.zeros((cols, LANES), jnp.float32)
    for j in range(halo_ids.shape[1]):
        ids = jnp.where(rows == j, ids_here[0, j].astype(jnp.float32), ids)
    ids = ids.astype(offered.dtype)
    for part in range(parts):
        offered[part, :, nodes:] = ids
    fetch_x.wait()
    own = x_here[...]
    for part in range(parts):
        offered[part, :, :nodes] = own


def terms_kernel(
    owners, subs, q_cols, xg, a_tiles, precisions, q_tiles, summed, window, weighted
):
    parts, cols, width = xg.shape
    obs_count, tile, _ = a_tiles.shape
    row_blocks, neighbours = q_cols.shape
    nodes = row_blocks * tile
    halo = (window.shape[0] - row_blocks) // len(OFFSETS)
    me = lax.axis_index("mesh")
    unroll = math.gcd(obs_count, UNROLL)

    def lanes_of(t):
        return pl.ds(pl.multiple_of(subs[t] * tile, tile), tile)

    def steps(step):
        if obs_count == unroll:
            step(0)
        else:
            pl.loop(0, obs_count // unroll)(step)

    summed[...] = jnp.zeros_like(summed)

    @steps
    def project(step):
        first = step * unroll
        scales = precisions[pl.ds(first, unroll), :].astype(jnp.float32)
        for u in range(unroll):
            t = first + u
            projected = lax.dot_general(
                xg[owners[t], :, lanes_of(t)], a_tiles[t], NT, preferred_element_type=jnp.float32
            )
            weighted[t] = (scales[u:u + 1, :] * projected).astype(jnp.bfloat16)

    for row in range(row_blocks):
        window[row] = xg[me, :, row * tile:(row + 1) * tile]
    for m, offset in enumerate(OFFSETS):
        part = lax.rem(me + offset + parts, parts)
        ids = xg[part, :, nodes:nodes + tile].astype(jnp.float32)
        for j in range(halo):
            wanted = jnp.broadcast_to(ids[j:j + 1, :], (cols, tile))
            picked = jnp.zeros((cols, tile), jnp.float32)
            for row in range(row_blocks):
                picked = jnp.where(
                    wanted == float(row),
                    xg[part, :, row * tile:(row + 1) * tile].astype(jnp.float32),
                    picked,
                )
            window[row_blocks + m * halo + j] = picked.astype(jnp.bfloat16)

    for row in range(row_blocks):
        total = None
        for k in range(neighbours):
            term = lax.dot_general(
                window[q_cols[row, k]], q_tiles[row * neighbours + k], NT,
                preferred_element_type=jnp.float32,
            )
            total = term if total is None else total + term
        summed[me, :, row * tile:(row + 1) * tile] = total

    @steps
    def spread(step):
        first = step * unroll
        made = [
            jnp.dot(weighted[first + u], a_tiles[first + u], preferred_element_type=jnp.float32)
            for u in range(unroll)
        ]
        for u in range(unroll):
            t = first + u
            summed[owners[t], :, lanes_of(t)] = summed[owners[t], :, lanes_of(t)] + made[u]


def over_parts(parts, step, carry):
    if parts > 16:
        return lax.fori_loop(0, parts, step, carry)
    for part in range(parts):
        carry = step(part, carry)
    return carry


def top_exponent(value):
    top = jnp.maximum(jnp.max(jnp.abs(value), axis=1, keepdims=True), 1e-30)
    return jnp.floor(jnp.log(32000.0 / top) * (1.0 / math.log(2.0)))


def power(exponent):
    return jnp.exp2(exponent)


def whole(value):
    return jnp.round(value).astype(jnp.int32).astype(jnp.int16)


def pair_products(summed, near, carry):
    parts, cols, nodes = summed.shape

    def add(part, carry):
        value = summed[part]
        high = value.astype(jnp.bfloat16)
        low = (value - high.astype(jnp.float32)).astype(jnp.bfloat16)
        out = []
        for ref, old in zip(near, carry):
            x = ref[part, :, :nodes]
            out.append(
                old
                + lax.dot_general(high, x, NT, preferred_element_type=jnp.float32)
                + lax.dot_general(low, x, NT, preferred_element_type=jnp.float32)
            )
        return tuple(out)

    return over_parts(parts, add, carry)


def at_column(piece, k):
    cols = piece.shape[0]
    wide = jnp.concatenate([piece, jnp.zeros((cols, LANES - cols), jnp.float32)], axis=1)
    return pltpu.roll(wide, lax.bitwise_xor(lax.axis_index("col"), k) * cols, 1)


def code_kernel(summed, near0, near1, near2, message, pairs, exponents):
    parts, cols, nodes = summed.shape

    def put(part, carry):
        value = summed[part]
        exponent = top_exponent(value)
        message[part, :, :nodes] = whole(value * power(exponent))
        exponents[part] = jnp.broadcast_to(exponent, (cols, LANES))
        return carry

    over_parts(parts, put, 0)
    zero = jnp.zeros((cols, cols), jnp.float32)
    pieces = pair_products(summed, (near0, near1, near2), (zero, zero, zero))
    pairs[...] = at_column(pieces[0], 0) + at_column(pieces[1], 1) + at_column(pieces[2], 2)


def gram_kernel(coded, pairs, exponents, summed, near3, message):
    parts, cols, nodes = summed.shape
    (piece,) = pair_products(summed, (near3,), (jnp.zeros((cols, cols), jnp.float32),))
    total = pairs[...] + at_column(piece, 3)
    quarter = LANES // 4
    lane = lax.broadcasted_iota(jnp.int32, (cols, LANES), 1)
    gram_exponent = top_exponent(total)
    scaled = total * power(gram_exponent)
    first = jnp.round(scaled)
    second = pltpu.roll((scaled - first) * 32768.0, quarter, 1)
    extra = jnp.where(lane < quarter, first, jnp.where(lane < 2 * quarter, second, gram_exponent))

    def put(part, carry):
        message[part, :, nodes:] = whole(jnp.where(lane < 3 * quarter, extra, exponents[part]))
        return carry

    over_parts(parts, put, 0)


def collect_kernel(summed, arrived, product, gram):
    parts, cols, nodes = summed.shape
    quarter = LANES // 4
    me = lax.axis_index("mesh")

    def add(part, carry):
        total, pairs = carry
        extra = arrived[part, :, nodes:].astype(jnp.int32).astype(jnp.float32)
        back = power(-extra[:, 3 * quarter:3 * quarter + 1])
        here = arrived[part, :, :nodes].astype(jnp.int32).astype(jnp.float32) * back
        total = total + jnp.where(part == me, summed[part], here)
        values = extra + pltpu.roll(extra, LANES - quarter, 1) * (1.0 / 32768.0)
        return total, pairs + values * power(-extra[:, 2 * quarter:2 * quarter + 1])

    start = jnp.zeros((cols, nodes), jnp.float32), jnp.zeros((cols, LANES), jnp.float32)
    total, pairs = over_parts(parts, add, start)
    product[...] = total
    gram[...] = pairs[:, :gram.shape[1]] * (1.0 / math.sqrt(nodes * parts))


def body(x_cols, q_tiles, q_cols, halo_ids, a_tiles, obs_prec, tile_owner, tile_sub):
    cols, nodes = x_cols.shape
    parts, groups = lax.axis_size("mesh"), lax.axis_size("col")
    obs_count, tile, _ = a_tiles.shape
    row_blocks = nodes // tile
    halo = halo_ids.shape[1]
    width = nodes + LANES
    vmem, smem = pl.BlockSpec(memory_space=pltpu.VMEM), pl.BlockSpec(memory_space=pltpu.SMEM)
    hbm = pl.BlockSpec(memory_space=pltpu.HBM)
    offered = pl.pallas_call(
        offer_kernel,
        out_shape=jax.ShapeDtypeStruct((parts, cols, width), x_cols.dtype),
        in_specs=[hbm, hbm],
        out_specs=vmem,
        scratch_shapes=[
            pltpu.SMEM(halo_ids.shape, jnp.int32),
            pltpu.VMEM(x_cols.shape, x_cols.dtype),
            pltpu.SemaphoreType.DMA((2,)),
        ],
        compiler_params=pltpu.CompilerParams(vmem_limit_bytes=GRANT),
        cost_estimate=pl.CostEstimate(
            flops=2_000_000_000, bytes_accessed=200_000, transcendentals=0
        ),
        name="offer",
    )(*(pltpu.with_memory_space_constraint(a, pltpu.HBM) for a in (halo_ids, x_cols)))
    xg = lax.all_to_all(offered, "mesh", 0, 0, tiled=True)
    def swap(array, k):
        return lax.ppermute(array, "col", [(i, i ^ k) for i in range(groups)])

    near2 = swap(xg, 2)
    near1 = swap(xg, 1)
    params = pltpu.CompilerParams(vmem_limit_bytes=GRANT)
    owners = tile_owner.reshape(-1)
    summed = pl.pallas_call(
        terms_kernel,
        out_shape=jax.ShapeDtypeStruct((parts, cols, nodes), jnp.float32),
        in_specs=[smem, smem, smem, vmem, vmem, vmem, vmem],
        out_specs=vmem,
        scratch_shapes=[
            pltpu.VMEM((row_blocks + len(OFFSETS) * halo, cols, tile), jnp.bfloat16),
            pltpu.VMEM((obs_count, cols, tile), jnp.bfloat16),
        ],
        compiler_params=params,
        cost_estimate=pl.CostEstimate(
            flops=100_000_000, bytes_accessed=4_000_000, transcendentals=0
        ),
        name="terms",
    )(owners, tile_sub, q_cols, xg, a_tiles, obs_prec, q_tiles)
    near2, summed = lax.optimization_barrier((near2, summed))
    near3 = swap(near2, 1)
    message_type = jax.ShapeDtypeStruct((parts, cols, width), jnp.int16)
    coded, pairs, exponents = pl.pallas_call(
        code_kernel,
        out_shape=[
            message_type,
            jax.ShapeDtypeStruct((cols, LANES), jnp.float32),
            jax.ShapeDtypeStruct((parts, cols, LANES), jnp.float32),
        ],
        in_specs=[vmem] * 4,
        out_specs=[vmem] * 3,
        compiler_params=params,
        cost_estimate=pl.CostEstimate(
            flops=30_000_000, bytes_accessed=1_000_000, transcendentals=0
        ),
        name="code",
    )(summed, xg, near1, near2)
    message = pl.pallas_call(
        gram_kernel,
        out_shape=message_type,
        in_specs=[pl.BlockSpec(memory_space=pl.ANY)] + [vmem] * 4,
        out_specs=vmem,
        input_output_aliases={0: 0},
        compiler_params=params,
        cost_estimate=pl.CostEstimate(
            flops=10_000_000, bytes_accessed=1_000_000, transcendentals=0
        ),
        name="gram",
    )(coded, pairs, exponents, summed, near3)
    arrived = lax.all_to_all(message, "mesh", 0, 0, tiled=True)
    product, gram = pl.pallas_call(
        collect_kernel,
        out_shape=[
            jax.ShapeDtypeStruct((cols, nodes), jnp.float32),
            jax.ShapeDtypeStruct((cols, groups * cols), jnp.float32),
        ],
        in_specs=[vmem, vmem],
        out_specs=[vmem, vmem],
        compiler_params=params,
        name="collect",
    )(summed, arrived)
    return product, gram.T


def solution(mesh):
    placed = (
        P("col", "mesh"),
        P("mesh", None, None),
        P("mesh", None),
        P("mesh", None),
        P("mesh", None, None),
        P("mesh", None),
        P("mesh", None),
        P("mesh"),
    )
    return jax.shard_map(
        body,
        mesh=mesh,
        in_specs=placed,
        out_specs=(P("col", "mesh"), P(None, "col")),
        check_vma=False,
    )
```

```python
import math

import jax
import jax.numpy as jnp
from jax import lax
from jax.experimental import pallas as pl
from jax.experimental.pallas import tpu as pltpu
from jax.sharding import PartitionSpec as P

OFFSETS = (-2, -1, 1, 2)
LANES = 128
NT = (((1,), (1,)), ((), ()))
UNROLL = 64
GRANT = 16 * 2**20


def offer_kernel(halo_ids, x_cols, offered, ids_here, x_here, sems):
    copies, _, width = offered.shape
    cols, nodes = x_cols.shape
    fetch_ids = pltpu.make_async_copy(halo_ids, ids_here, sems.at[0])
    fetch_x = pltpu.make_async_copy(x_cols, x_here, sems.at[1])
    fetch_ids.start()
    fetch_x.start()
    fetch_ids.wait()
    rows = lax.broadcasted_iota(jnp.int32, (cols, LANES), 0)
    ids = jnp.zeros((cols, LANES), jnp.float32)
    for j in range(halo_ids.shape[1]):
        ids = jnp.where(rows == j, ids_here[0, j].astype(jnp.float32), ids)
    ids = ids.astype(offered.dtype)
    for copy in range(copies):
        offered[copy, :, nodes:] = ids
    fetch_x.wait()
    own = x_here[...]
    for copy in range(copies):
        offered[copy, :, :nodes] = own


def terms_kernel(
    owners, subs, q_cols, xg, a_tiles, precisions, q_tiles, summed, window, weighted
):
    parts, cols, width = xg.shape
    obs_count, tile, _ = a_tiles.shape
    row_blocks, neighbours = q_cols.shape
    nodes = row_blocks * tile
    halo = (window.shape[0] - row_blocks) // len(OFFSETS)
    me = lax.axis_index("mesh")
    unroll = math.gcd(obs_count, UNROLL)

    def lanes_of(t):
        return pl.ds(pl.multiple_of(subs[t] * tile, tile), tile)

    def steps(step):
        if obs_count == unroll:
            step(0)
        else:
            pl.loop(0, obs_count // unroll)(step)

    summed[...] = jnp.zeros_like(summed)

    @steps
    def project(step):
        first = step * unroll
        scales = precisions[pl.ds(first, unroll), :].astype(jnp.float32)
        for u in range(unroll):
            t = first + u
            projected = lax.dot_general(
                xg[owners[t], :, lanes_of(t)], a_tiles[t], NT, preferred_element_type=jnp.float32
            )
            weighted[t] = (scales[u:u + 1, :] * projected).astype(jnp.bfloat16)

    for row in range(row_blocks):
        window[row] = xg[me, :, row * tile:(row + 1) * tile]
    for m, offset in enumerate(OFFSETS):
        part = lax.rem(me + offset + parts, parts)
        ids = xg[part, :, nodes:nodes + tile].astype(jnp.float32)
        for j in range(halo):
            wanted = jnp.broadcast_to(ids[j:j + 1, :], (cols, tile))
            picked = jnp.zeros((cols, tile), jnp.float32)
            for row in range(row_blocks):
                picked = jnp.where(
                    wanted == float(row),
                    xg[part, :, row * tile:(row + 1) * tile].astype(jnp.float32),
                    picked,
                )
            window[row_blocks + m * halo + j] = picked.astype(jnp.bfloat16)

    for row in range(row_blocks):
        total = None
        for k in range(neighbours):
            term = lax.dot_general(
                window[q_cols[row, k]], q_tiles[row * neighbours + k], NT,
                preferred_element_type=jnp.float32,
            )
            total = term if total is None else total + term
        summed[me, :, row * tile:(row + 1) * tile] = total

    @steps
    def spread(step):
        first = step * unroll
        made = [
            jnp.dot(weighted[first + u], a_tiles[first + u], preferred_element_type=jnp.float32)
            for u in range(unroll)
        ]
        for u in range(unroll):
            t = first + u
            summed[owners[t], :, lanes_of(t)] = summed[owners[t], :, lanes_of(t)] + made[u]


def over_parts(parts, step, carry):
    if parts > 16:
        return lax.fori_loop(0, parts, step, carry)
    for part in range(parts):
        carry = step(part, carry)
    return carry


def top_exponent(value):
    top = jnp.maximum(jnp.max(jnp.abs(value), axis=1, keepdims=True), 1e-30)
    return jnp.floor(jnp.log(32000.0 / top) * (1.0 / math.log(2.0)))


def power(exponent):
    return jnp.exp2(exponent)


def whole(value):
    return jnp.round(value).astype(jnp.int32).astype(jnp.int16)


def pair_products(summed, near):
    parts, cols, nodes = summed.shape

    def add(part, total):
        value = summed[part]
        high = value.astype(jnp.bfloat16)
        low = (value - high.astype(jnp.float32)).astype(jnp.bfloat16)
        x = [array[part, :, :nodes] for array in near]
        return total + lax.dot_general(
            jnp.concatenate([high, low], axis=0),
            x[0] if len(x) == 1 else jnp.concatenate(x, axis=0),
            NT,
            preferred_element_type=jnp.float32,
        )

    total = over_parts(parts, add, jnp.zeros((2 * cols, len(near) * cols), jnp.float32))
    total = total[:cols] + total[cols:]
    return [total[:, k * cols:(k + 1) * cols] for k in range(len(near))]


def at_column(piece, k):
    cols = piece.shape[0]
    wide = jnp.concatenate([piece, jnp.zeros((cols, LANES - cols), jnp.float32)], axis=1)
    return pltpu.roll(wide, lax.bitwise_xor(lax.axis_index("col"), k) * cols, 1)


def code_kernel(summed, near0, near1, near2, message, pairs, exponents):
    parts, cols, nodes = summed.shape

    def put(part, carry):
        value = summed[part]
        exponent = top_exponent(value)
        message[part, :, :nodes] = whole(value * power(exponent))
        exponents[part] = jnp.broadcast_to(exponent, (cols, LANES))
        return carry

    over_parts(parts, put, 0)
    pieces = pair_products(summed, (near0, near1, near2))
    pairs[...] = at_column(pieces[0], 0) + at_column(pieces[1], 1) + at_column(pieces[2], 2)


def gram_kernel(coded, pairs, exponents, summed, near3, message):
    parts, cols, nodes = summed.shape
    (piece,) = pair_products(summed, (near3,))
    total = pairs[...] + at_column(piece, 3)
    quarter = LANES // 4
    lane = lax.broadcasted_iota(jnp.int32, (cols, LANES), 1)
    gram_exponent = top_exponent(total)
    scaled = total * power(gram_exponent)
    first = jnp.round(scaled)
    second = pltpu.roll((scaled - first) * 32768.0, quarter, 1)
    extra = jnp.where(lane < quarter, first, jnp.where(lane < 2 * quarter, second, gram_exponent))

    def put(part, carry):
        message[part, :, nodes:] = whole(jnp.where(lane < 3 * quarter, extra, exponents[part]))
        return carry

    over_parts(parts, put, 0)


def collect_kernel(summed, arrived, product, gram):
    parts, cols, nodes = summed.shape
    quarter = LANES // 4
    me = lax.axis_index("mesh")

    def add(part, carry):
        total, pairs = carry
        extra = arrived[part, :, nodes:].astype(jnp.int32).astype(jnp.float32)
        back = power(-extra[:, 3 * quarter:3 * quarter + 1])
        here = arrived[part, :, :nodes].astype(jnp.int32).astype(jnp.float32) * back
        total = total + jnp.where(part == me, summed[part], here)
        values = extra + pltpu.roll(extra, LANES - quarter, 1) * (1.0 / 32768.0)
        return total, pairs + values * power(-extra[:, 2 * quarter:2 * quarter + 1])

    start = jnp.zeros((cols, nodes), jnp.float32), jnp.zeros((cols, LANES), jnp.float32)
    total, pairs = over_parts(parts, add, start)
    product[...] = total
    gram[...] = pairs[:, :gram.shape[1]] * (1.0 / math.sqrt(nodes * parts))


def body(x_cols, q_tiles, q_cols, halo_ids, a_tiles, obs_prec, tile_owner, tile_sub):
    cols, nodes = x_cols.shape
    parts, groups = lax.axis_size("mesh"), lax.axis_size("col")
    obs_count, tile, _ = a_tiles.shape
    row_blocks = nodes // tile
    halo = halo_ids.shape[1]
    width = nodes + LANES

    def swap(array, k):
        return lax.ppermute(array, "col", [(i, i ^ k) for i in range(groups)])

    vmem, smem = pl.BlockSpec(memory_space=pltpu.VMEM), pl.BlockSpec(memory_space=pltpu.SMEM)
    hbm = pl.BlockSpec(memory_space=pltpu.HBM)
    params = pltpu.CompilerParams(vmem_limit_bytes=GRANT)

    def run(kernel, name, flops, out_shape, *arrays, in_specs=None, **rest):
        return pl.pallas_call(
            kernel,
            out_shape=out_shape,
            in_specs=in_specs or [vmem] * len(arrays),
            out_specs=jax.tree.map(lambda _: vmem, out_shape),
            compiler_params=params,
            cost_estimate=pl.CostEstimate(
                flops=flops, bytes_accessed=1_000_000, transcendentals=0
            ),
            name=name,
            **rest,
        )(*arrays)

    def x_type(count, lanes=width):
        return jax.ShapeDtypeStruct((count, cols, lanes), x_cols.dtype)

    offered = run(
        offer_kernel,
        "offer",
        2_000_000_000,
        x_type(parts),
        *(pltpu.with_memory_space_constraint(a, pltpu.HBM) for a in (halo_ids, x_cols)),
        in_specs=[hbm, hbm],
        scratch_shapes=[
            pltpu.SMEM(halo_ids.shape, jnp.int32),
            pltpu.VMEM(x_cols.shape, x_cols.dtype),
            pltpu.SemaphoreType.DMA((2,)),
        ],
    )
    xg = lax.all_to_all(offered, "mesh", 0, 0, tiled=True)
    near2 = swap(xg, 2)
    near1 = swap(xg, 1)
    owners = tile_owner.reshape(-1)
    summed = run(
        terms_kernel,
        "terms",
        100_000_000,
        jax.ShapeDtypeStruct((parts, cols, nodes), jnp.float32),
        owners, tile_sub, q_cols, xg, a_tiles, obs_prec, q_tiles,
        in_specs=[smem] * 3 + [vmem] * 4,
        scratch_shapes=[
            pltpu.VMEM((row_blocks + len(OFFSETS) * halo, cols, tile), jnp.bfloat16),
            pltpu.VMEM((obs_count, cols, tile), jnp.bfloat16),
        ],
    )
    near2, summed = lax.optimization_barrier((near2, summed))
    near3 = swap(near2, 1)
    message_type = jax.ShapeDtypeStruct((parts, cols, width), jnp.int16)
    coded, pairs, exponents = run(
        code_kernel,
        "code",
        30_000_000,
        [
            message_type,
            jax.ShapeDtypeStruct((cols, LANES), jnp.float32),
            jax.ShapeDtypeStruct((parts, cols, LANES), jnp.float32),
        ],
        summed, xg, near1, near2,
    )
    message = run(
        gram_kernel,
        "gram",
        10_000_000,
        message_type,
        coded, pairs, exponents, summed, near3,
        in_specs=[pl.BlockSpec(memory_space=pl.ANY)] + [vmem] * 4,
        input_output_aliases={0: 0},
    )
    arrived = lax.all_to_all(message, "mesh", 0, 0, tiled=True)
    product, gram = run(
        collect_kernel,
        "collect",
        1_000_000,
        [
            jax.ShapeDtypeStruct((cols, nodes), jnp.float32),
            jax.ShapeDtypeStruct((cols, groups * cols), jnp.float32),
        ],
        summed, arrived,
    )
    return product, gram.T


def solution(mesh):
    placed = (
        P("col", "mesh"),
        P("mesh", None, None),
        P("mesh", None),
        P("mesh", None),
        P("mesh", None, None),
        P("mesh", None),
        P("mesh", None),
        P("mesh"),
    )
    return jax.shard_map(
        body,
        mesh=mesh,
        in_specs=placed,
        out_specs=(P("col", "mesh"), P(None, "col")),
        check_vma=False,
    )
```

```python
import math

import jax
import jax.numpy as jnp
from jax import lax
from jax.experimental import pallas as pl
from jax.experimental.pallas import tpu as pltpu
from jax.sharding import PartitionSpec as P

OFFSETS = (-2, -1, 1, 2)
LANES = 128
NT = (((1,), (1,)), ((), ()))
UNROLL = 64
GRANT = 16 * 2**20


def offer_kernel(halo_ids, x_cols, offered, ids_here, x_here, sems):
    copies, _, width = offered.shape
    cols, nodes = x_cols.shape
    fetch_ids = pltpu.make_async_copy(halo_ids, ids_here, sems.at[0])
    fetch_x = pltpu.make_async_copy(x_cols, x_here, sems.at[1])
    fetch_ids.start()
    fetch_x.start()
    fetch_ids.wait()
    rows = lax.broadcasted_iota(jnp.int32, (cols, LANES), 0)
    ids = jnp.zeros((cols, LANES), jnp.float32)
    for j in range(halo_ids.shape[1]):
        ids = jnp.where(rows == j, ids_here[0, j].astype(jnp.float32), ids)
    ids = ids.astype(offered.dtype)
    for copy in range(copies):
        offered[copy, :, nodes:] = ids
    fetch_x.wait()
    own = x_here[...]
    for copy in range(copies):
        offered[copy, :, :nodes] = own


def stay_kernel(offered, same):
    del offered, same


def trim_kernel(xg, x):
    def put(part, carry):
        x[part] = xg[part, :, :x.shape[2]]
        return carry

    over_parts(x.shape[0], put, 0)


def terms_kernel(
    owners, subs, q_cols, xg, a_tiles, precisions, q_tiles, summed, window, weighted
):
    parts, cols, width = xg.shape
    obs_count, tile, _ = a_tiles.shape
    row_blocks, neighbours = q_cols.shape
    nodes = row_blocks * tile
    halo = (window.shape[0] - row_blocks) // len(OFFSETS)
    me = lax.axis_index("mesh")
    unroll = math.gcd(obs_count, UNROLL)

    def lanes_of(t):
        return pl.ds(pl.multiple_of(subs[t] * tile, tile), tile)

    def steps(step):
        if obs_count == unroll:
            step(0)
        else:
            pl.loop(0, obs_count // unroll)(step)

    summed[...] = jnp.zeros_like(summed)

    @steps
    def project(step):
        first = step * unroll
        scales = precisions[pl.ds(first, unroll), :].astype(jnp.float32)
        for u in range(unroll):
            t = first + u
            projected = lax.dot_general(
                xg[owners[t], :, lanes_of(t)], a_tiles[t], NT, preferred_element_type=jnp.float32
            )
            weighted[t] = (scales[u:u + 1, :] * projected).astype(jnp.bfloat16)

    for row in range(row_blocks):
        window[row] = xg[me, :, row * tile:(row + 1) * tile]
    for m, offset in enumerate(OFFSETS):
        part = lax.rem(me + offset + parts, parts)
        ids = xg[part, :, nodes:nodes + tile].astype(jnp.float32)
        for j in range(halo):
            wanted = jnp.broadcast_to(ids[j:j + 1, :], (cols, tile))
            picked = jnp.zeros((cols, tile), jnp.float32)
            for row in range(row_blocks):
                picked = jnp.where(
                    wanted == float(row),
                    xg[part, :, row * tile:(row + 1) * tile].astype(jnp.float32),
                    picked,
                )
            window[row_blocks + m * halo + j] = picked.astype(jnp.bfloat16)

    for row in range(row_blocks):
        total = None
        for k in range(neighbours):
            term = lax.dot_general(
                window[q_cols[row, k]], q_tiles[row * neighbours + k], NT,
                preferred_element_type=jnp.float32,
            )
            total = term if total is None else total + term
        summed[me, :, row * tile:(row + 1) * tile] = total

    @steps
    def spread(step):
        first = step * unroll
        made = [
            jnp.dot(weighted[first + u], a_tiles[first + u], preferred_element_type=jnp.float32)
            for u in range(unroll)
        ]
        for u in range(unroll):
            t = first + u
            summed[owners[t], :, lanes_of(t)] = summed[owners[t], :, lanes_of(t)] + made[u]


def over_parts(parts, step, carry):
    if parts > 16:
        return lax.fori_loop(0, parts, step, carry)
    for part in range(parts):
        carry = step(part, carry)
    return carry


def top_exponent(value):
    top = jnp.maximum(jnp.max(jnp.abs(value), axis=1, keepdims=True), 1e-30)
    return jnp.floor(jnp.log(32000.0 / top) * (1.0 / math.log(2.0)))


def power(exponent):
    return jnp.exp2(exponent)


def whole(value):
    return jnp.round(value).astype(jnp.int32).astype(jnp.int16)


def pair_products(summed, near):
    parts, cols, nodes = summed.shape

    def add(part, total):
        value = summed[part]
        high = value.astype(jnp.bfloat16)
        low = (value - high.astype(jnp.float32)).astype(jnp.bfloat16)
        x = [array[part, :, :nodes] for array in near]
        return total + lax.dot_general(
            jnp.concatenate([high, low], axis=0),
            x[0] if len(x) == 1 else jnp.concatenate(x, axis=0),
            NT,
            preferred_element_type=jnp.float32,
        )

    total = over_parts(parts, add, jnp.zeros((2 * cols, len(near) * cols), jnp.float32))
    total = total[:cols] + total[cols:]
    return [total[:, k * cols:(k + 1) * cols] for k in range(len(near))]


def at_column(piece, k):
    cols = piece.shape[0]
    wide = jnp.concatenate([piece, jnp.zeros((cols, LANES - cols), jnp.float32)], axis=1)
    return pltpu.roll(wide, lax.bitwise_xor(lax.axis_index("col"), k) * cols, 1)


def code_kernel(summed, near0, near1, near2, message, pairs, exponents):
    parts, cols, nodes = summed.shape

    def put(part, carry):
        value = summed[part]
        exponent = top_exponent(value)
        message[part, :, :nodes] = whole(value * power(exponent))
        exponents[part] = jnp.broadcast_to(exponent, (cols, LANES))
        return carry

    over_parts(parts, put, 0)
    pieces = pair_products(summed, (near0, near1, near2))
    pairs[...] = at_column(pieces[0], 0) + at_column(pieces[1], 1) + at_column(pieces[2], 2)


def gram_kernel(coded, pairs, exponents, summed, near3, message):
    parts, cols, nodes = summed.shape
    (piece,) = pair_products(summed, (near3,))
    total = pairs[...] + at_column(piece, 3)
    quarter = LANES // 4
    lane = lax.broadcasted_iota(jnp.int32, (cols, LANES), 1)
    gram_exponent = top_exponent(total)
    scaled = total * power(gram_exponent)
    first = jnp.round(scaled)
    second = pltpu.roll((scaled - first) * 32768.0, quarter, 1)
    extra = jnp.where(lane < quarter, first, jnp.where(lane < 2 * quarter, second, gram_exponent))

    def put(part, carry):
        message[part, :, nodes:] = whole(jnp.where(lane < 3 * quarter, extra, exponents[part]))
        return carry

    over_parts(parts, put, 0)


def collect_kernel(summed, arrived, product, gram):
    parts, cols, nodes = summed.shape
    quarter = LANES // 4
    me = lax.axis_index("mesh")

    def add(part, carry):
        total, pairs = carry
        extra = arrived[part, :, nodes:].astype(jnp.int32).astype(jnp.float32)
        back = power(-extra[:, 3 * quarter:3 * quarter + 1])
        here = arrived[part, :, :nodes].astype(jnp.int32).astype(jnp.float32) * back
        total = total + jnp.where(part == me, summed[part], here)
        values = extra + pltpu.roll(extra, LANES - quarter, 1) * (1.0 / 32768.0)
        return total, pairs + values * power(-extra[:, 2 * quarter:2 * quarter + 1])

    start = jnp.zeros((cols, nodes), jnp.float32), jnp.zeros((cols, LANES), jnp.float32)
    total, pairs = over_parts(parts, add, start)
    product[...] = total
    gram[...] = pairs[:, :gram.shape[1]] * (1.0 / math.sqrt(nodes * parts))


def body(x_cols, q_tiles, q_cols, halo_ids, a_tiles, obs_prec, tile_owner, tile_sub):
    cols, nodes = x_cols.shape
    parts, groups = lax.axis_size("mesh"), lax.axis_size("col")
    obs_count, tile, _ = a_tiles.shape
    row_blocks = nodes // tile
    halo = halo_ids.shape[1]
    width = nodes + LANES

    def swap(array, k):
        return lax.ppermute(array, "col", [(i, i ^ k) for i in range(groups)])

    vmem, smem = pl.BlockSpec(memory_space=pltpu.VMEM), pl.BlockSpec(memory_space=pltpu.SMEM)
    hbm = pl.BlockSpec(memory_space=pltpu.HBM)
    params = pltpu.CompilerParams(vmem_limit_bytes=GRANT)

    def run(kernel, name, flops, out_shape, *arrays, in_specs=None, out_specs=None, **rest):
        return pl.pallas_call(
            kernel,
            out_shape=out_shape,
            in_specs=in_specs or [vmem] * len(arrays),
            out_specs=out_specs or jax.tree.map(lambda _: vmem, out_shape),
            compiler_params=params,
            cost_estimate=pl.CostEstimate(
                flops=flops, bytes_accessed=1_000_000, transcendentals=0
            ),
            name=name,
            **rest,
        )(*arrays)

    def x_type(count, lanes=width):
        return jax.ShapeDtypeStruct((count, cols, lanes), x_cols.dtype)

    offered = run(
        offer_kernel,
        "offer",
        1_000,
        x_type(parts),
        *(pltpu.with_memory_space_constraint(a, pltpu.HBM) for a in (halo_ids, x_cols)),
        in_specs=[hbm, hbm],
        scratch_shapes=[
            pltpu.SMEM(halo_ids.shape, jnp.int32),
            pltpu.VMEM(x_cols.shape, x_cols.dtype),
            pltpu.SemaphoreType.DMA((2,)),
        ],
    )
    offered = run(
        stay_kernel,
        "stay",
        2_000_000_000,
        x_type(parts),
        offered,
        in_specs=[pl.BlockSpec(memory_space=pl.ANY)],
        input_output_aliases={0: 0},
        out_specs=pl.BlockSpec(memory_space=pl.ANY),
    )
    xg = lax.all_to_all(offered, "mesh", 0, 0, tiled=True)
    near0 = run(trim_kernel, "trim", 1_000_000, x_type(parts, nodes), xg)
    near2 = swap(near0, 2)
    near1 = swap(near0, 1)
    owners = tile_owner.reshape(-1)
    summed = run(
        terms_kernel,
        "terms",
        100_000_000,
        jax.ShapeDtypeStruct((parts, cols, nodes), jnp.float32),
        owners, tile_sub, q_cols, xg, a_tiles, obs_prec, q_tiles,
        in_specs=[smem] * 3 + [vmem] * 4,
        scratch_shapes=[
            pltpu.VMEM((row_blocks + len(OFFSETS) * halo, cols, tile), jnp.bfloat16),
            pltpu.VMEM((obs_count, cols, tile), jnp.bfloat16),
        ],
    )
    near2, summed = lax.optimization_barrier((near2, summed))
    near3 = swap(near2, 1)
    message_type = jax.ShapeDtypeStruct((parts, cols, width), jnp.int16)
    coded, pairs, exponents = run(
        code_kernel,
        "code",
        30_000_000,
        [
            message_type,
            jax.ShapeDtypeStruct((cols, LANES), jnp.float32),
            jax.ShapeDtypeStruct((parts, cols, LANES), jnp.float32),
        ],
        summed, near0, near1, near2,
    )
    message = run(
        gram_kernel,
        "gram",
        10_000_000,
        message_type,
        coded, pairs, exponents, summed, near3,
        in_specs=[pl.BlockSpec(memory_space=pl.ANY)] + [vmem] * 4,
        input_output_aliases={0: 0},
    )
    arrived = lax.all_to_all(message, "mesh", 0, 0, tiled=True)
    product, gram = run(
        collect_kernel,
        "collect",
        1_000_000,
        [
            jax.ShapeDtypeStruct((cols, nodes), jnp.float32),
            jax.ShapeDtypeStruct((cols, groups * cols), jnp.float32),
        ],
        summed, arrived,
    )
    return product, gram.T


def solution(mesh):
    placed = (
        P("col", "mesh"),
        P("mesh", None, None),
        P("mesh", None),
        P("mesh", None),
        P("mesh", None, None),
        P("mesh", None),
        P("mesh", None),
        P("mesh"),
    )
    return jax.shard_map(
        body,
        mesh=mesh,
        in_specs=placed,
        out_specs=(P("col", "mesh"), P(None, "col")),
        check_vma=False,
    )
```

```python
import math

import jax
import jax.numpy as jnp
from jax import lax
from jax.experimental import pallas as pl
from jax.experimental.pallas import tpu as pltpu
from jax.sharding import PartitionSpec as P

OFFSETS = (-2, -1, 1, 2)
LANES = 128
NT = (((1,), (1,)), ((), ()))
UNROLL = 64
GRANT = 16 * 2**20


def offer_kernel(halo_ids, x_cols, offered, ids_here, x_here, sems):
    copies, _, width = offered.shape
    cols, nodes = x_cols.shape
    fetch_ids = pltpu.make_async_copy(halo_ids, ids_here, sems.at[0])
    fetch_x = pltpu.make_async_copy(x_cols, x_here, sems.at[1])
    fetch_ids.start()
    fetch_x.start()
    fetch_ids.wait()
    rows = lax.broadcasted_iota(jnp.int32, (cols, LANES), 0)
    ids = jnp.zeros((cols, LANES), jnp.float32)
    for j in range(halo_ids.shape[1]):
        ids = jnp.where(rows == j, ids_here[0, j].astype(jnp.float32), ids)
    ids = ids.astype(offered.dtype)
    for copy in range(copies):
        offered[copy, :, nodes:] = ids
    fetch_x.wait()
    own = x_here[...]
    for copy in range(copies):
        offered[copy, :, :nodes] = own


def stay_kernel(offered, same):
    del offered, same


def trim_kernel(xg, x):
    def put(part, carry):
        x[part] = xg[part, :, :x.shape[2]]
        return carry

    over_parts(x.shape[0], put, 0)


def terms_kernel(
    owners, subs, q_cols, xg, a_tiles, precisions, q_tiles, summed, window, weighted
):
    parts, cols, width = xg.shape
    obs_count, tile, _ = a_tiles.shape
    row_blocks, neighbours = q_cols.shape
    nodes = row_blocks * tile
    halo = (window.shape[0] - row_blocks) // len(OFFSETS)
    me = lax.axis_index("mesh")
    unroll = math.gcd(obs_count, UNROLL)

    def lanes_of(t):
        return pl.ds(pl.multiple_of(subs[t] * tile, tile), tile)

    def steps(step):
        if obs_count == unroll:
            step(0)
        else:
            pl.loop(0, obs_count // unroll)(step)

    summed[...] = jnp.zeros_like(summed)

    @steps
    def project(step):
        first = step * unroll
        scales = precisions[pl.ds(first, unroll), :].astype(jnp.float32)
        for u in range(unroll):
            t = first + u
            projected = lax.dot_general(
                xg[owners[t], :, lanes_of(t)], a_tiles[t], NT, preferred_element_type=jnp.float32
            )
            weighted[t] = (scales[u:u + 1, :] * projected).astype(jnp.bfloat16)

    for row in range(row_blocks):
        window[row] = xg[me, :, row * tile:(row + 1) * tile]
    for m, offset in enumerate(OFFSETS):
        part = lax.rem(me + offset + parts, parts)
        ids = xg[part, :, nodes:nodes + tile].astype(jnp.float32)
        for j in range(halo):
            wanted = jnp.broadcast_to(ids[j:j + 1, :], (cols, tile))
            picked = jnp.zeros((cols, tile), jnp.float32)
            for row in range(row_blocks):
                picked = jnp.where(
                    wanted == float(row),
                    xg[part, :, row * tile:(row + 1) * tile].astype(jnp.float32),
                    picked,
                )
            window[row_blocks + m * halo + j] = picked.astype(jnp.bfloat16)

    for row in range(row_blocks):
        total = None
        for k in range(neighbours):
            term = lax.dot_general(
                window[q_cols[row, k]], q_tiles[row * neighbours + k], NT,
                preferred_element_type=jnp.float32,
            )
            total = term if total is None else total + term
        summed[me, :, row * tile:(row + 1) * tile] = total

    @steps
    def spread(step):
        first = step * unroll
        made = [
            jnp.dot(weighted[first + u], a_tiles[first + u], preferred_element_type=jnp.float32)
            for u in range(unroll)
        ]
        for u in range(unroll):
            t = first + u
            summed[owners[t], :, lanes_of(t)] = summed[owners[t], :, lanes_of(t)] + made[u]


def over_parts(parts, step, carry):
    if parts > 16:
        return lax.fori_loop(0, parts, step, carry)
    for part in range(parts):
        carry = step(part, carry)
    return carry


def top_exponent(value):
    top = jnp.maximum(jnp.max(jnp.abs(value), axis=1, keepdims=True), 1e-30)
    return jnp.floor(jnp.log(32000.0 / top) * (1.0 / math.log(2.0)))


def power(exponent):
    return jnp.exp2(exponent)


def whole(value):
    return jnp.round(value).astype(jnp.int32).astype(jnp.int16)


def stacked(value):
    high = value.astype(jnp.bfloat16)
    low = (value - high.astype(jnp.float32)).astype(jnp.bfloat16)
    return jnp.concatenate([high, low], axis=0)


def pair_products(parts, left, near):
    cols, nodes = near[0].shape[1], left(0).shape[1]

    def add(part, total):
        x = [array[part, :, :nodes] for array in near]
        return total + lax.dot_general(
            left(part),
            x[0] if len(x) == 1 else jnp.concatenate(x, axis=0),
            NT,
            preferred_element_type=jnp.float32,
        )

    total = over_parts(parts, add, jnp.zeros((2 * cols, len(near) * cols), jnp.float32))
    total = total[:cols] + total[cols:]
    return [total[:, k * cols:(k + 1) * cols] for k in range(len(near))]


def at_column(piece, k):
    cols = piece.shape[0]
    wide = jnp.concatenate([piece, jnp.zeros((cols, LANES - cols), jnp.float32)], axis=1)
    return pltpu.roll(wide, lax.bitwise_xor(lax.axis_index("col"), k) * cols, 1)


def code_kernel(summed, near0, near1, near2, message, pairs, exponents, halves):
    parts, cols, nodes = summed.shape

    def put(part, carry):
        value = summed[part]
        exponent = top_exponent(value)
        message[part, :, :nodes] = whole(value * power(exponent))
        exponents[part] = jnp.broadcast_to(exponent, (cols, LANES))
        halves[part] = stacked(value)
        return carry

    over_parts(parts, put, 0)
    pieces = pair_products(parts, lambda part: stacked(summed[part]), (near0, near1, near2))
    pairs[...] = at_column(pieces[0], 0) + at_column(pieces[1], 1) + at_column(pieces[2], 2)


def gram_kernel(coded, pairs, exponents, halves, near3, message):
    parts, cols, _ = exponents.shape
    nodes = halves.shape[2]
    (piece,) = pair_products(parts, lambda part: halves[part], (near3,))
    total = pairs[...] + at_column(piece, 3)
    quarter = LANES // 4
    lane = lax.broadcasted_iota(jnp.int32, (cols, LANES), 1)
    gram_exponent = top_exponent(total)
    scaled = total * power(gram_exponent)
    first = jnp.round(scaled)
    second = pltpu.roll((scaled - first) * 32768.0, quarter, 1)
    extra = jnp.where(lane < quarter, first, jnp.where(lane < 2 * quarter, second, gram_exponent))

    def put(part, carry):
        message[part, :, nodes:] = whole(jnp.where(lane < 3 * quarter, extra, exponents[part]))
        return carry

    over_parts(parts, put, 0)


def collect_kernel(summed, arrived, product, gram):
    parts, cols, nodes = summed.shape
    quarter = LANES // 4
    me = lax.axis_index("mesh")

    def add(part, carry):
        total, pairs = carry
        extra = arrived[part, :, nodes:].astype(jnp.int32).astype(jnp.float32)
        back = power(-extra[:, 3 * quarter:3 * quarter + 1])
        here = arrived[part, :, :nodes].astype(jnp.int32).astype(jnp.float32) * back
        total = total + jnp.where(part == me, summed[part], here)
        values = extra + pltpu.roll(extra, LANES - quarter, 1) * (1.0 / 32768.0)
        return total, pairs + values * power(-extra[:, 2 * quarter:2 * quarter + 1])

    start = jnp.zeros((cols, nodes), jnp.float32), jnp.zeros((cols, LANES), jnp.float32)
    total, pairs = over_parts(parts, add, start)
    product[...] = total
    gram[...] = pairs[:, :gram.shape[1]] * (1.0 / math.sqrt(nodes * parts))


def body(x_cols, q_tiles, q_cols, halo_ids, a_tiles, obs_prec, tile_owner, tile_sub):
    cols, nodes = x_cols.shape
    parts, groups = lax.axis_size("mesh"), lax.axis_size("col")
    obs_count, tile, _ = a_tiles.shape
    row_blocks = nodes // tile
    halo = halo_ids.shape[1]
    width = nodes + LANES

    def swap(array, k):
        return lax.ppermute(array, "col", [(i, i ^ k) for i in range(groups)])

    vmem, smem = pl.BlockSpec(memory_space=pltpu.VMEM), pl.BlockSpec(memory_space=pltpu.SMEM)
    hbm = pl.BlockSpec(memory_space=pltpu.HBM)
    params = pltpu.CompilerParams(vmem_limit_bytes=GRANT)

    def run(kernel, name, flops, out_shape, *arrays, in_specs=None, out_specs=None, **rest):
        return pl.pallas_call(
            kernel,
            out_shape=out_shape,
            in_specs=in_specs or [vmem] * len(arrays),
            out_specs=out_specs or jax.tree.map(lambda _: vmem, out_shape),
            compiler_params=params,
            cost_estimate=pl.CostEstimate(
                flops=flops, bytes_accessed=1_000_000, transcendentals=0
            ),
            name=name,
            **rest,
        )(*arrays)

    def x_type(count, lanes=width):
        return jax.ShapeDtypeStruct((count, cols, lanes), x_cols.dtype)

    offered = run(
        offer_kernel,
        "offer",
        1_000,
        x_type(parts),
        *(pltpu.with_memory_space_constraint(a, pltpu.HBM) for a in (halo_ids, x_cols)),
        in_specs=[hbm, hbm],
        scratch_shapes=[
            pltpu.SMEM(halo_ids.shape, jnp.int32),
            pltpu.VMEM(x_cols.shape, x_cols.dtype),
            pltpu.SemaphoreType.DMA((2,)),
        ],
    )
    offered = run(
        stay_kernel,
        "stay",
        2_000_000_000,
        x_type(parts),
        offered,
        in_specs=[pl.BlockSpec(memory_space=pl.ANY)],
        input_output_aliases={0: 0},
        out_specs=pl.BlockSpec(memory_space=pl.ANY),
    )
    xg = lax.all_to_all(offered, "mesh", 0, 0, tiled=True)
    near0 = run(trim_kernel, "trim", 1_000_000, x_type(parts, nodes), xg)
    near2 = swap(near0, 2)
    near1 = swap(near0, 1)
    owners = tile_owner.reshape(-1)
    summed = run(
        terms_kernel,
        "terms",
        100_000_000,
        jax.ShapeDtypeStruct((parts, cols, nodes), jnp.float32),
        owners, tile_sub, q_cols, xg, a_tiles, obs_prec, q_tiles,
        in_specs=[smem] * 3 + [vmem] * 4,
        scratch_shapes=[
            pltpu.VMEM((row_blocks + len(OFFSETS) * halo, cols, tile), jnp.bfloat16),
            pltpu.VMEM((obs_count, cols, tile), jnp.bfloat16),
        ],
    )
    near2, summed = lax.optimization_barrier((near2, summed))
    near3 = swap(near2, 1)
    message_type = jax.ShapeDtypeStruct((parts, cols, width), jnp.int16)
    coded, pairs, exponents, halves = run(
        code_kernel,
        "code",
        30_000_000,
        [
            message_type,
            jax.ShapeDtypeStruct((cols, LANES), jnp.float32),
            jax.ShapeDtypeStruct((parts, cols, LANES), jnp.float32),
            jax.ShapeDtypeStruct((parts, 2 * cols, nodes), jnp.bfloat16),
        ],
        summed, near0, near1, near2,
    )
    message = run(
        gram_kernel,
        "gram",
        10_000_000,
        message_type,
        coded, pairs, exponents, halves, near3,
        in_specs=[pl.BlockSpec(memory_space=pl.ANY)] + [vmem] * 4,
        input_output_aliases={0: 0},
    )
    arrived = lax.all_to_all(message, "mesh", 0, 0, tiled=True)
    product, gram = run(
        collect_kernel,
        "collect",
        1_000_000,
        [
            jax.ShapeDtypeStruct((cols, nodes), jnp.float32),
            jax.ShapeDtypeStruct((cols, groups * cols), jnp.float32),
        ],
        summed, arrived,
    )
    return product, gram.T


def solution(mesh):
    placed = (
        P("col", "mesh"),
        P("mesh", None, None),
        P("mesh", None),
        P("mesh", None),
        P("mesh", None, None),
        P("mesh", None),
        P("mesh", None),
        P("mesh"),
    )
    return jax.shard_map(
        body,
        mesh=mesh,
        in_specs=placed,
        out_specs=(P("col", "mesh"), P(None, "col")),
        check_vma=False,
    )
```

```python
import math

import jax
import jax.numpy as jnp
from jax import lax
from jax.experimental import pallas as pl
from jax.experimental.pallas import tpu as pltpu
from jax.sharding import PartitionSpec as P

OFFSETS = (-2, -1, 1, 2)
LANES = 128
NT = (((1,), (1,)), ((), ()))
UNROLL = 64
GRANT = 16 * 2**20


def offer_kernel(halo_ids, x_cols, offered, ids_here, x_here, sems):
    copies, _, width = offered.shape
    cols, nodes = x_cols.shape
    fetch_ids = pltpu.make_async_copy(halo_ids, ids_here, sems.at[0])
    fetch_x = pltpu.make_async_copy(x_cols, x_here, sems.at[1])
    fetch_ids.start()
    fetch_x.start()
    fetch_ids.wait()
    rows = lax.broadcasted_iota(jnp.int32, (cols, LANES), 0)
    ids = jnp.zeros((cols, LANES), jnp.float32)
    for j in range(halo_ids.shape[1]):
        ids = jnp.where(rows == j, ids_here[0, j].astype(jnp.float32), ids)
    ids = ids.astype(offered.dtype)
    for copy in range(copies):
        offered[copy, :, nodes:] = ids
    fetch_x.wait()
    own = x_here[...]
    for copy in range(copies):
        offered[copy, :, :nodes] = own


def trim_kernel(xg, x):
    def put(part, carry):
        x[part] = xg[part, :, :x.shape[2]]
        return carry

    over_parts(x.shape[0], put, 0)


def terms_kernel(
    owners, subs, q_cols, xg, a_tiles, precisions, q_tiles, summed, window, weighted
):
    parts, cols, width = xg.shape
    obs_count, tile, _ = a_tiles.shape
    row_blocks, neighbours = q_cols.shape
    nodes = row_blocks * tile
    halo = (window.shape[0] - row_blocks) // len(OFFSETS)
    me = lax.axis_index("mesh")
    unroll = math.gcd(obs_count, UNROLL)

    def lanes_of(t):
        return pl.ds(pl.multiple_of(subs[t] * tile, tile), tile)

    def steps(step):
        if obs_count == unroll:
            step(0)
        else:
            pl.loop(0, obs_count // unroll)(step)

    summed[...] = jnp.zeros_like(summed)

    @steps
    def project(step):
        first = step * unroll
        scales = precisions[pl.ds(first, unroll), :].astype(jnp.float32)
        for u in range(unroll):
            t = first + u
            projected = lax.dot_general(
                xg[owners[t], :, lanes_of(t)], a_tiles[t], NT, preferred_element_type=jnp.float32
            )
            weighted[t] = (scales[u:u + 1, :] * projected).astype(jnp.bfloat16)

    for row in range(row_blocks):
        window[row] = xg[me, :, row * tile:(row + 1) * tile]
    for m, offset in enumerate(OFFSETS):
        part = lax.rem(me + offset + parts, parts)
        ids = xg[part, :, nodes:nodes + tile].astype(jnp.float32)
        for j in range(halo):
            wanted = jnp.broadcast_to(ids[j:j + 1, :], (cols, tile))
            picked = jnp.zeros((cols, tile), jnp.float32)
            for row in range(row_blocks):
                picked = jnp.where(
                    wanted == float(row),
                    xg[part, :, row * tile:(row + 1) * tile].astype(jnp.float32),
                    picked,
                )
            window[row_blocks + m * halo + j] = picked.astype(jnp.bfloat16)

    for row in range(row_blocks):
        total = None
        for k in range(neighbours):
            term = lax.dot_general(
                window[q_cols[row, k]], q_tiles[row * neighbours + k], NT,
                preferred_element_type=jnp.float32,
            )
            total = term if total is None else total + term
        summed[me, :, row * tile:(row + 1) * tile] = total

    @steps
    def spread(step):
        first = step * unroll
        made = [
            jnp.dot(weighted[first + u], a_tiles[first + u], preferred_element_type=jnp.float32)
            for u in range(unroll)
        ]
        for u in range(unroll):
            t = first + u
            summed[owners[t], :, lanes_of(t)] = summed[owners[t], :, lanes_of(t)] + made[u]


def over_parts(parts, step, carry):
    if parts > 16:
        return lax.fori_loop(0, parts, step, carry)
    for part in range(parts):
        carry = step(part, carry)
    return carry


def top_exponent(value):
    top = jnp.maximum(jnp.max(jnp.abs(value), axis=1, keepdims=True), 1e-30)
    return jnp.floor(jnp.log(32000.0 / top) * (1.0 / math.log(2.0)))


def power(exponent):
    return jnp.exp2(exponent)


def whole(value):
    return jnp.round(value).astype(jnp.int32).astype(jnp.int16)


def pair_products(summed, near):
    parts, cols, nodes = summed.shape

    def add(part, total):
        value = summed[part]
        high = value.astype(jnp.bfloat16)
        low = (value - high.astype(jnp.float32)).astype(jnp.bfloat16)
        x = [array[part, :, :nodes] for array in near]
        return total + lax.dot_general(
            jnp.concatenate([high, low], axis=0),
            x[0] if len(x) == 1 else jnp.concatenate(x, axis=0),
            NT,
            preferred_element_type=jnp.float32,
        )

    total = over_parts(parts, add, jnp.zeros((2 * cols, len(near) * cols), jnp.float32))
    total = total[:cols] + total[cols:]
    return [total[:, k * cols:(k + 1) * cols] for k in range(len(near))]


def at_column(piece, k):
    cols = piece.shape[0]
    wide = jnp.concatenate([piece, jnp.zeros((cols, LANES - cols), jnp.float32)], axis=1)
    return pltpu.roll(wide, lax.bitwise_xor(lax.axis_index("col"), k) * cols, 1)


def code_kernel(summed, near0, near1, near2, message, pairs, exponents):
    parts, cols, nodes = summed.shape

    def put(part, carry):
        value = summed[part]
        exponent = top_exponent(value)
        message[part, :, :nodes] = whole(value * power(exponent))
        exponents[part] = jnp.broadcast_to(exponent, (cols, LANES))
        return carry

    over_parts(parts, put, 0)
    pieces = pair_products(summed, (near0, near1, near2))
    pairs[...] = at_column(pieces[0], 0) + at_column(pieces[1], 1) + at_column(pieces[2], 2)


def gram_kernel(coded, pairs, exponents, summed, near3, message):
    parts, cols, nodes = summed.shape
    (piece,) = pair_products(summed, (near3,))
    total = pairs[...] + at_column(piece, 3)
    quarter = LANES // 4
    lane = lax.broadcasted_iota(jnp.int32, (cols, LANES), 1)
    gram_exponent = top_exponent(total)
    scaled = total * power(gram_exponent)
    first = jnp.round(scaled)
    second = pltpu.roll((scaled - first) * 32768.0, quarter, 1)
    extra = jnp.where(lane < quarter, first, jnp.where(lane < 2 * quarter, second, gram_exponent))

    def put(part, carry):
        message[part, :, nodes:] = whole(jnp.where(lane < 3 * quarter, extra, exponents[part]))
        return carry

    over_parts(parts, put, 0)


def collect_kernel(summed, arrived, product, gram):
    parts, cols, nodes = summed.shape
    quarter = LANES // 4
    me = lax.axis_index("mesh")

    def add(part, carry):
        total, pairs = carry
        extra = arrived[part, :, nodes:].astype(jnp.int32).astype(jnp.float32)
        back = power(-extra[:, 3 * quarter:3 * quarter + 1])
        here = arrived[part, :, :nodes].astype(jnp.int32).astype(jnp.float32) * back
        total = total + jnp.where(part == me, summed[part], here)
        values = extra + pltpu.roll(extra, LANES - quarter, 1) * (1.0 / 32768.0)
        return total, pairs + values * power(-extra[:, 2 * quarter:2 * quarter + 1])

    start = jnp.zeros((cols, nodes), jnp.float32), jnp.zeros((cols, LANES), jnp.float32)
    total, pairs = over_parts(parts, add, start)
    product[...] = total
    gram[...] = pairs[:, :gram.shape[1]] * (1.0 / math.sqrt(nodes * parts))


def body(x_cols, q_tiles, q_cols, halo_ids, a_tiles, obs_prec, tile_owner, tile_sub):
    cols, nodes = x_cols.shape
    parts, groups = lax.axis_size("mesh"), lax.axis_size("col")
    obs_count, tile, _ = a_tiles.shape
    row_blocks = nodes // tile
    halo = halo_ids.shape[1]
    width = nodes + LANES

    def swap(array, k):
        return lax.ppermute(array, "col", [(i, i ^ k) for i in range(groups)])

    vmem, smem = pl.BlockSpec(memory_space=pltpu.VMEM), pl.BlockSpec(memory_space=pltpu.SMEM)
    hbm = pl.BlockSpec(memory_space=pltpu.HBM)
    params = pltpu.CompilerParams(vmem_limit_bytes=GRANT)

    def run(kernel, name, flops, out_shape, *arrays, in_specs=None, out_specs=None, **rest):
        return pl.pallas_call(
            kernel,
            out_shape=out_shape,
            in_specs=in_specs or [vmem] * len(arrays),
            out_specs=out_specs or jax.tree.map(lambda _: vmem, out_shape),
            compiler_params=params,
            cost_estimate=pl.CostEstimate(
                flops=flops, bytes_accessed=1_000_000, transcendentals=0
            ),
            name=name,
            **rest,
        )(*arrays)

    def x_type(count, lanes=width):
        return jax.ShapeDtypeStruct((count, cols, lanes), x_cols.dtype)

    offered = run(
        offer_kernel,
        "offer",
        2_000_000_000,
        x_type(parts),
        *(pltpu.with_memory_space_constraint(a, pltpu.HBM) for a in (halo_ids, x_cols)),
        in_specs=[hbm, hbm],
        scratch_shapes=[
            pltpu.SMEM(halo_ids.shape, jnp.int32),
            pltpu.VMEM(x_cols.shape, x_cols.dtype),
            pltpu.SemaphoreType.DMA((2,)),
        ],
    )
    xg = lax.all_to_all(offered, "mesh", 0, 0, tiled=True)
    near0 = run(trim_kernel, "trim", 1_000_000, x_type(parts, nodes), xg)
    near2 = swap(near0, 2)
    near1 = swap(near0, 1)
    owners = tile_owner.reshape(-1)
    summed = run(
        terms_kernel,
        "terms",
        100_000_000,
        jax.ShapeDtypeStruct((parts, cols, nodes), jnp.float32),
        owners, tile_sub, q_cols, xg, a_tiles, obs_prec, q_tiles,
        in_specs=[smem] * 3 + [vmem] * 4,
        scratch_shapes=[
            pltpu.VMEM((row_blocks + len(OFFSETS) * halo, cols, tile), jnp.bfloat16),
            pltpu.VMEM((obs_count, cols, tile), jnp.bfloat16),
        ],
    )
    near2, summed = lax.optimization_barrier((near2, summed))
    near3 = swap(near2, 1)
    message_type = jax.ShapeDtypeStruct((parts, cols, width), jnp.int16)
    coded, pairs, exponents = run(
        code_kernel,
        "code",
        30_000_000,
        [
            message_type,
            jax.ShapeDtypeStruct((cols, LANES), jnp.float32),
            jax.ShapeDtypeStruct((parts, cols, LANES), jnp.float32),
        ],
        summed, near0, near1, near2,
    )
    message = run(
        gram_kernel,
        "gram",
        10_000_000,
        message_type,
        coded, pairs, exponents, summed, near3,
        in_specs=[pl.BlockSpec(memory_space=pl.ANY)] + [vmem] * 4,
        input_output_aliases={0: 0},
    )
    arrived = lax.all_to_all(message, "mesh", 0, 0, tiled=True)
    product, gram = run(
        collect_kernel,
        "collect",
        1_000_000,
        [
            jax.ShapeDtypeStruct((cols, nodes), jnp.float32),
            jax.ShapeDtypeStruct((cols, groups * cols), jnp.float32),
        ],
        summed, arrived,
    )
    return product, gram.T


def solution(mesh):
    placed = (
        P("col", "mesh"),
        P("mesh", None, None),
        P("mesh", None),
        P("mesh", None),
        P("mesh", None, None),
        P("mesh", None),
        P("mesh", None),
        P("mesh"),
    )
    return jax.shard_map(
        body,
        mesh=mesh,
        in_specs=placed,
        out_specs=(P("col", "mesh"), P(None, "col")),
        check_vma=False,
    )
```
